16 devices in a mesh: dp: 2 (over y, z), tp: 8 (over x, core).
Axes of the slice: x: 4, y: 2, z: 1, core: 2. Of those that a mesh axis runs over, the one named last changes fastest.
The devices are a block of a 4x4x8 slice.
Arguments:
- X: bfloat16 [8192, 4096], P('dp'), parts along dimension 0
- W: bfloat16 [4096, 32768], P(None, 'tp')
- labels: int32 [8192], P('dp'), parts along dimension 0
Outputs:
- output 1: float32 [2], P('dp'), parts along dimension 0
- output 2: bfloat16 [8192, 32768], P('dp', 'tp'), parts along dimension 0
- output 3: bfloat16 [8192, 4096], P('dp'), parts along dimension 0
There are 2 independent parts. The reference program is written for one: setup_inputs(seed, part) draws one part's arguments, and reference() takes and returns one part's arrays. A program takes and returns all parts, laid end to end along the dimension named above; an argument that names none is the same for every part.
All inputs are finite; a program needn't handle non-finite values.
Results may differ from the reference program's by a relative error of at most 0.001.
Values are sent between devices in bfloat16 or wider.
A program may use at most 768 MiB of HBM per device.

```python
import math

import jax
import jax.numpy as jnp
from jax import lax

T = 4096
H = 4096
V = 32768


def setup_inputs(seed: int = 0, part: int = 0) -> dict:
    key = jax.random.PRNGKey(seed)
    kshared, kpart = jax.random.split(key)
    kp = jax.random.fold_in(kpart, part)
    kx, kl, kc, ku, kv, kg = jax.random.split(kp, 6)
    nb = 4
    Wf = jax.random.normal(kshared, (H, V), jnp.float32) * H ** -0.5
    kl1, kl2 = jax.random.split(jax.random.fold_in(kl, 7))
    la = jax.random.randint(kl1, (T,), 0, V // 16, jnp.int32)
    lb = jax.random.randint(kl2, (T,), 0, V, jnp.int32)
    labels = jnp.where(jnp.arange(T) % 2 == 0, la, lb)
    cols = jax.random.randint(kc, (T, nb), 0, V, jnp.int32)
    amp = math.log(V) + jax.random.uniform(ku, (T, nb), jnp.float32, 0.0, 2.5)
    amp_label = (math.log(V) + jax.random.uniform(kv, (T,), jnp.float32, -2.0, 2.0)
                 + jax.random.uniform(kg, (), jnp.float32, -1.0, 1.0))
    X = jax.random.normal(kx, (T, H), jnp.float32)
    for k in range(nb):
        X = X + amp[:, k:k + 1] * Wf[:, cols[:, k]].T
    X = X + amp_label[:, None] * Wf[:, labels].T
    return {'X': X.astype(jnp.bfloat16), 'W': Wf.astype(jnp.bfloat16), 'labels': labels}


def reference(X, W, labels):
    VC = min(V, 2048)
    nb = V // VC
    Wb = W.reshape(H, nb, VC).transpose(1, 0, 2)
    offs = jnp.arange(nb, dtype=jnp.int32) * VC
    cols = jnp.arange(VC, dtype=jnp.int32)

    def stats(a):
        w, off = a
        z = jnp.dot(X, w, preferred_element_type=jnp.float32)
        m = z.max(axis=1)
        s = jnp.exp(z - m[:, None]).sum(axis=1)
        hit = (cols[None, :] + off) == labels[:, None]
        t = jnp.where(hit, z, 0.0).sum(axis=1)
        return m, s, t

    m, s, t = lax.map(stats, (Wb, offs))
    M = m.max(axis=0)
    S = (s * jnp.exp(m - M[None, :])).sum(axis=0)
    zt = t.sum(axis=0)
    L = jnp.mean(M + jnp.log(S) - zt).reshape(1)

    def back(dx, a):
        w, off = a
        z = jnp.dot(X, w, preferred_element_type=jnp.float32)
        hit = (cols[None, :] + off) == labels[:, None]
        g = ((jnp.exp(z - M[:, None]) / S[:, None] - hit.astype(jnp.float32)) / T).astype(jnp.bfloat16)
        dw = jnp.dot(X.T, g, preferred_element_type=jnp.float32).astype(jnp.bfloat16)
        dx = dx + jnp.dot(g, w.T, preferred_element_type=jnp.float32)
        return dx, dw

    dx, dWb = lax.scan(back, jnp.zeros((T, H), jnp.float32), (Wb, offs))
    dW = dWb.transpose(1, 0, 2).reshape(H, V)
    return (L, dW, dx.astype(jnp.bfloat16))
```

```python
import functools

import jax
import jax.numpy as jnp
from jax import lax
from jax.experimental import pallas as pl
from jax.experimental.pallas import tpu as pltpu
from jax.sharding import PartitionSpec as P

TB = 512
CN = 512
PERIOD = 6
OFFS = (0, 1, 2, 3, 5, 6, 8, 10)


def kernel(n, X, W, lab, Lo, dW, dX, Gh, Q, rA, rB, rC,
           wg, xb, gb, prs, st_send, st_recv, va, vq, vs, vt, ro,
           wsem, xsem, lsem, gsem, stS, stR, cred, psS, psR, qsem, xssem, odsem,
           aS, aR, bS, bR, cS, cR, gS, gR, rS, rR, sS, sR, ldsem, rosem):
    T, H = X.shape
    V = W.shape[1]
    NB, NV = T // TB, V // CN
    HH = H // 2
    ND = HH // CN
    NU = 2 * NB
    UR = TB // 2
    nc = n // 2
    QR = UR // nc
    HR = QR // 2
    f32, bf16 = jnp.float32, jnp.bfloat16
    me = lax.axis_index('tp')
    core = me % 2
    chip = me // 2
    sib = chip * 2 + 1 - core
    cn, cp, cf = (chip + 1) % nc, (chip + nc - 1) % nc, (chip + 2) % nc
    nxt, prv = cn * 2 + core, cp * 2 + core
    off = me * V

    def rcopy(src, dst, ss, rs, dev):
        return pltpu.make_async_remote_copy(src_ref=src, dst_ref=dst, send_sem=ss, recv_sem=rs,
                                            device_id={'tp': dev}, device_id_type=pl.DeviceIdType.MESH)

    def lcopy(src, dst, sem):
        return pltpu.make_async_copy(src, dst, sem)

    def mo(x, m):
        return x if isinstance(x, int) else pl.multiple_of(x, m)

    def cols(j):
        return pl.ds(mo(j * CN, CN), CN)

    def xcopy(b):
        return lcopy(X.at[pl.ds(mo(b * TB, TB), TB)], xb, xsem)

    def wcopy(j):
        return lcopy(W.at[:, cols(j)], wg.at[:, cols(j)], wsem.at[j])

    def qrows(u, c, h):
        return Q.at[pl.ds(mo(u * UR + c * QR + h * HR, HR), HR)]

    def rrows(r, d, u):
        return r.at[d, pl.ds(mo(u * HR, HR), HR)]

    def xrows(u, c, h, rows, k):
        return dX.at[pl.ds(mo(u * UR + c * QR + h * HR, HR), rows), pl.ds(mo(k * HH, HH), HH)]

    def sendA(u, d):
        return rcopy(qrows(u, cf, d), rrows(rA, d, u), aS.at[d], aR.at[d, u], (nxt, prv)[d])

    def sendB(u, d):
        return rcopy(qrows(u, (cn, cp)[d], 1 - d), rrows(rB, d, u), bS.at[d], bR.at[d, u], (nxt, prv)[d])

    def sendC(u, d):
        return rcopy(va.at[d], rrows(rC, d, u), cS.at[d], cR.at[d, u], (nxt, prv)[d])

    def loadC(u):
        return ([lcopy(rrows(rA, d, u), va.at[d], ldsem.at[d]) for d in (0, 1)]
                + [lcopy(qrows(u, (cn, cp)[d], d), vq.at[d], ldsem.at[2 + d]) for d in (0, 1)])

    def loadS(u):
        return ([lcopy(qrows(u, chip, h), vs.at[h], ldsem.at[4 + h]) for h in (0, 1)]
                + [lcopy(rrows(rC, h, u), vt.at[0, h], ldsem.at[6 + h]) for h in (0, 1)]
                + [lcopy(rrows(rB, 1 - h, u), vt.at[1, h], ldsem.at[8 + h]) for h in (0, 1)])

    def sendG(u, d):
        return rcopy(ro, xrows(u, chip, 0, QR, core), gS.at[d], gR.at[d, u], (nxt, prv)[d])

    def recvG(u, d):
        return rcopy(ro, xrows(u, (cp, cn)[d], 0, QR, core), gS.at[d], gR.at[d, u], (nxt, prv)[d])

    def sendR(u, d):
        r = xrows(u, (cp, cn)[d], d, HR, core)
        return rcopy(r, r, rS.at[d], rR.at[d, u], (nxt, prv)[d])

    def recvR(u, d):
        r = xrows(u, cf, d, HR, core)
        return rcopy(r, r, rS.at[d], rR.at[d, u], (nxt, prv)[d])

    def sibO(u):
        return rcopy(ro, xrows(u, chip, 0, QR, core), sS.at[0], sR.at[u], sib)

    def sibG(u, d):
        r = xrows(u, (cp, cn)[d], 0, QR, core)
        return rcopy(r, r, sS.at[1 + d], sR.at[u], sib)

    def sibR(u):
        r = xrows(u, cf, 0, QR, core)
        return rcopy(r, r, sS.at[3], sR.at[u], sib)

    def sibW(u):
        r = dX.at[pl.ds(mo(u * UR, UR), UR), pl.ds(mo((1 - core) * HH, HH), HH)]
        return rcopy(r, r, sS.at[0], sR.at[u], sib)

    def ownO(u):
        return lcopy(ro, xrows(u, chip, 0, QR, core), rosem)

    def st0(u):
        @pl.when(u > 0)
        def _():
            for d in (0, 1):
                sendA(u - 1, d).wait_send()
        for d in (0, 1):
            sendA(u, d).start()

    def st1(u):
        @pl.when(u > 0)
        def _():
            for d in (0, 1):
                sendB(u - 1, d).wait_send()
        for d in (0, 1):
            sendB(u, d).start()

    def st2(u):
        @pl.when(u > 0)
        def _():
            for d in (0, 1):
                sendC(u - 1, d).wait_send()
        for d in (0, 1):
            sendA(u, d).wait_recv()
        for c in loadC(u):
            c.start()

    def st3(u):
        for c in loadC(u):
            c.wait()
        va[...] = va[...] + vq[...]
        for d in (0, 1):
            sendC(u, d).start()

    def st4(u):
        for d in (0, 1):
            sendB(u, d).wait_recv()
            sendC(u, d).wait_recv()
        for c in loadS(u):
            c.start()

    def st5(u):
        @pl.when(u > 0)
        def _():
            for d in (0, 1):
                sendG(u - 1, d).wait_send()
            sibO(u - 1).wait_send()
            ownO(u - 1).wait()
        for c in loadS(u):
            c.wait()
        for h in (0, 1):
            ro[h * HR:(h + 1) * HR] = ((vt[0, h] + vs[h]) + vt[1, h]).astype(bf16)
        for d in (0, 1):
            sendG(u, d).start()
        ownO(u).start()
        sibO(u).start()

    def st6(u):
        @pl.when(u > 0)
        def _():
            for d in (0, 1):
                sendR(u - 1, d).wait_send()
                sibG(u - 1, d).wait_send()
        for d in (0, 1):
            recvG(u, d).wait_recv()
        for d in (0, 1):
            sendR(u, d).start()
        for d in (0, 1):
            sibG(u, d).start()

    def st7(u):
        @pl.when(u > 0)
        def _():
            sibR(u - 1).wait_send()
        for d in (0, 1):
            recvR(u, d).wait_recv()
        sibR(u).start()

    ST = NV // 2
    K0 = 3 * ST

    def exchange(k):
        for o, fn in reversed(tuple(zip(OFFS, (st0, st1, st2, st3, st4, st5, st6, st7)))):
            t = k - (K0 + o)
            u = t // PERIOD

            @pl.when((t >= 0) & (t % PERIOD == 0) & (u < NU))
            def _(fn=fn, u=u):
                fn(u)

    barrier = pltpu.get_barrier_semaphore()
    for i in range(1, n):
        pl.semaphore_signal(barrier, inc=1, device_id={'tp': (me + i) % n}, device_id_type=pl.DeviceIdType.MESH)
    pl.semaphore_wait(barrier, n - 1)
    xcopy(0).start()
    for j in range(NV):
        wcopy(j).start()

    def stat_copy(par, i):
        peer = (me + i) % n
        return rcopy(st_send.at[par], st_recv.at[par, me], stS.at[par, i], stR.at[par, me], peer)

    def stat_recv(par, i):
        src = (me + n - i) % n
        return rcopy(st_send.at[par], st_recv.at[par, src], stS.at[par, i], stR.at[par, src], src)

    def gcopy(b):
        return lcopy(gb, Gh.at[pl.ds(mo(b * TB, TB), TB)], gsem.at[0])

    def phase1(eb, za, zb, ps, qs, lb, m_run, s_run, z_run, mjs, lacc):
        RT = min(64, TB)
        lane = lax.broadcasted_iota(jnp.int32, (RT, 128), 1)
        laneT = lax.broadcasted_iota(jnp.int32, (TB, 128), 1)

        def lcp(b):
            return lcopy(lab.at[pl.ds(mo(b * TB, TB), TB)], lb.at[b % 2], lsem)

        lcp(0).start()
        lacc[...] = jnp.zeros_like(lacc)

        def zdot(j, z):
            z[...] = jnp.dot(xb[...], wg[:, cols(j)], preferred_element_type=f32)

        def epi(z, j, par):
            base = j * CN
            for r in range(0, TB, RT):
                rows = slice(r, r + RT)
                zq = [z[rows, q * 128:(q + 1) * 128] for q in range(CN // 128)]
                mx = functools.reduce(jnp.maximum, zq)
                m_old = m_run[rows]
                m_new = jnp.maximum(m_old, jnp.max(mx, axis=1, keepdims=True))
                m_run[rows] = m_new
                mjs[rows] = jnp.where(lane == j, m_new, mjs[rows])
                s = s_run[rows] * jnp.exp(m_old - m_new)
                t = z_run[rows]
                lb_r = lb[par, rows] - (off + base)
                for q in range(CN // 128):
                    e = jnp.exp(zq[q] - m_new)
                    eb[j, rows, q * 128:(q + 1) * 128] = e
                    s = s + e
                    t = t + jnp.where(lane + q * 128 == lb_r, zq[q], 0.0)
                s_run[rows] = s
                z_run[rows] = t

        def zphase(b):
            par = b % 2
            xcopy(b).wait()
            lcp(b).wait()
            m_run[...] = jnp.full_like(m_run, -jnp.inf)
            s_run[...] = jnp.zeros_like(s_run)
            z_run[...] = jnp.zeros_like(z_run)
            mjs[...] = jnp.zeros_like(mjs)

            def wwait(j):
                @pl.when(b == 0)
                def _():
                    wcopy(j).wait()

            wwait(0)
            zdot(0, za)

            def body(i, c):
                exchange(2 * ST * b - ST + i)
                wwait(2 * i + 1)
                wwait(2 * i + 2)
                zdot(2 * i + 1, zb)
                epi(za, 2 * i, par)
                zdot(2 * i + 2, za)
                epi(zb, 2 * i + 1, par)
                return c

            lax.fori_loop(0, NV // 2 - 1, body, 0)
            exchange(2 * ST * b - 1)
            wwait(NV - 1)
            zdot(NV - 1, zb)
            epi(za, NV - 2, par)

            @pl.when(b < NB - 1)
            def _():
                xcopy(b + 1).start()
            epi(zb, NV - 1, par)

        def send_stats(b):
            par = b % 2
            s = jnp.sum(s_run[...], axis=1, keepdims=True)
            t = jnp.sum(z_run[...], axis=1, keepdims=True)
            a = jnp.where(laneT == 0, m_run[...], jnp.where(laneT == 1, s, jnp.where(laneT == 2, t, 0.0)))
            at = a.T[0:8]

            @pl.when(b >= 2)
            def _():
                for i in range(1, n):
                    stat_copy(par, i).wait_send()
            st_send[par] = at
            st_recv[par, me] = at
            for i in range(1, n):
                stat_copy(par, i).start()

        def gpass(b):
            par = b % 2
            for i in range(1, n):
                stat_recv(par, i).wait_recv()
            ms = [st_recv[par, i, 0:1] for i in range(n)]
            M = functools.reduce(jnp.maximum, ms)
            S = sum(st_recv[par, i, 1:2] * jnp.exp(ms[i] - M) for i in range(n))
            zt = sum(st_recv[par, i, 2:3] for i in range(n))
            lacc[...] = lacc[...] + ((M + jnp.log(S)) - zt)
            sub = lax.broadcasted_iota(jnp.int32, (128, TB), 0)
            bt = jnp.where(sub == 0, M, jnp.where(sub == 1, 1.0 / S, 0.0)).T
            R = jnp.exp(mjs[...] - bt[:, 0:1]) * bt[:, 1:2]
            mjs[...] = R

            @pl.when(b > 0)
            def _():
                gcopy(b - 1).wait()

            def body(j, c):
                for r in range(0, TB, RT):
                    rows = slice(r, r + RT)
                    rj = jnp.sum(jnp.where(lane == j, mjs[rows], 0.0), axis=1, keepdims=True)
                    lb_r = lb[par, rows] - (off + j * CN)
                    for q in range(CN // 128):
                        e = eb[j, rows, q * 128:(q + 1) * 128] * rj
                        e = (e - jnp.where(lane + q * 128 == lb_r, 1.0, 0.0)) * (1.0 / T)
                        gb[rows, pl.ds(mo(j * CN + q * 128, 128), 128)] = e.astype(bf16)
                return c

            lax.fori_loop(0, NV, body, 0)
            gcopy(b).start()

        def dxdot(row0):
            return lax.dot_general(gb[...], wg[pl.ds(mo(row0, CN), CN), :], (((1,), (1,)), ((), ())),
                                   preferred_element_type=f32)

        def pscopy(j, s):
            return rcopy(ps.at[s], prs.at[j], psS.at[s], psR.at[j], sib)

        def qcopy(b, j, s):
            return lcopy(qs.at[s], Q.at[pl.ds(mo(b * TB, TB), TB), cols(j)], qsem.at[s])

        def dxphase(b, k0):
            def body_s(i, c):
                exchange(k0 + i)
                for s in (0, 1):
                    j = 2 * i + s

                    @pl.when(i > 0)
                    def _(j=j, s=s):
                        pscopy(j - 2, s).wait_send()
                    ps[s] = dxdot((1 - core) * HH + j * CN)

                    @pl.when(b > 0)
                    def _(j=j):
                        pl.semaphore_wait(cred.at[j], 1)
                    pscopy(j, s).start()
                return c

            lax.fori_loop(0, ND // 2, body_s, 0)

            def body_o(i, c):
                exchange(k0 + ND // 2 + i)
                for s in (0, 1):
                    j = 2 * i + s

                    @pl.when(i > 0)
                    def _(j=j, s=s):
                        qcopy(b, j - 2, s).wait()
                    pscopy(j, s).wait_recv()
                    qs[s] = dxdot(core * HH + j * CN) + prs[j]
                    qcopy(b, j, s).start()

                    @pl.when(b < NB - 1)
                    def _(j=j):
                        pl.semaphore_signal(cred.at[j], inc=1, device_id={'tp': sib},
                                            device_id_type=pl.DeviceIdType.MESH)
                return c

            lax.fori_loop(0, ND // 2, body_o, 0)
            for s in (0, 1):
                pscopy(ND - 2 + s, s).wait_send()

        def block(b, c):
            @pl.when(b < NB)
            def _():
                zphase(b)
                send_stats(b)

                @pl.when(b < NB - 1)
                def _():
                    lcp(b + 1).start()

            @pl.when(b == NB)
            def _():
                for i in range(T // TB):
                    x0copy(i).start()

            @pl.when(b > 0)
            def _():
                dxphase(b - 1, jnp.minimum(2 * ST * b, (2 * NB - 1) * ST))

            @pl.when(b < NB)
            def _():
                gpass(b)

            @pl.when(b > 0)
            def _():
                for s in (0, 1):
                    qcopy(b - 1, ND - 2 + s, s).wait()
            return c

        lax.fori_loop(0, NB + 1, block, 0)
        for b in (NB - 2, NB - 1):
            for i in range(1, n):
                stat_copy(b % 2, i).wait_send()
        Lo[...] = jnp.zeros_like(Lo) + jnp.sum(lacc[...], axis=1, keepdims=True) * (1.0 / T)

    def x0copy(i):
        return lcopy(X.at[pl.ds(i * TB, TB), pl.ds(0, TB)], xb.at[:, pl.ds(i * TB, TB)], wsem.at[i])

    pl.run_scoped(phase1,
                  pltpu.VMEM((NV, TB, CN), f32), pltpu.VMEM((TB, CN), f32), pltpu.VMEM((TB, CN), f32),
                  pltpu.VMEM((2, TB, CN), f32), pltpu.VMEM((2, TB, CN), f32), pltpu.VMEM((2, TB, 128), jnp.int32),
                  pltpu.VMEM((TB, 128), f32), pltpu.VMEM((TB, 128), f32), pltpu.VMEM((TB, 128), f32),
                  pltpu.VMEM((TB, 128), f32), pltpu.VMEM((1, TB), f32))

    KD = 2 * ST * NB
    NH = H // TB

    def phase2(xs, od):
        SL = T // (NV // 2)

        def gload(j):
            return lcopy(Gh.at[:, cols(j)], wg.at[:, cols(j)], gsem.at[j])

        def xscopy(h, i):
            return lcopy(X.at[pl.ds(mo(i * SL, SL), SL), pl.ds(mo(h * TB, TB), TB)], xs.at[i % 2], xssem.at[i % 2])

        def odcopy(h, j, s):
            return lcopy(od.at[s], dW.at[pl.ds(mo(h * TB, TB), TB), cols(j)], odsem.at[s])

        gcopy(NB - 1).wait()
        for j in range(NV):
            gload(j).start()
        xscopy(1, 0).start()
        for i in range(T // TB):
            x0copy(i).wait()

        def tr0(i, c):
            gb[:, pl.ds(mo(i * TB, TB), TB)] = xb[:, pl.ds(mo(i * TB, TB), TB)].T
            return c

        lax.fori_loop(0, T // TB, tr0, 0)

        def hstep(h, cur, fut):
            def body(i, c):
                exchange(KD + h * (NV // 2) + i)

                @pl.when(h == 0)
                def _():
                    gload(2 * i).wait()
                    gload(2 * i + 1).wait()

                @pl.when((h > 0) | (i > 0))
                def _():
                    for s in (0, 1):
                        odcopy(h, 2 * i + s, s).wait()
                hn = jnp.minimum(h + 1, NH - 1)
                xscopy(hn, i).wait()

                @pl.when((h < NH - 1) | (i < NV // 2 - 1))
                def _():
                    last = i == NV // 2 - 1
                    xscopy(jnp.minimum(jnp.where(last, h + 2, h + 1), NH - 1), jnp.where(last, 0, i + 1)).start()
                for s in (0, 1):
                    od[s] = jnp.dot(cur[...], wg[:, cols(2 * i + s)], preferred_element_type=f32).astype(bf16)
                fut[:, pl.ds(mo(i * SL, SL), SL)] = xs[i % 2].T
                for s in (0, 1):
                    odcopy(h, 2 * i + s, s).start()
                return c

            lax.fori_loop(0, NV // 2, body, 0)

        def hpair(hh, c):
            hstep(2 * hh, gb, xb)
            hstep(2 * hh + 1, xb, gb)
            return c

        lax.fori_loop(0, NH // 2, hpair, 0)
        for s in (0, 1):
            odcopy(NH - 1, NV - 2 + s, s).wait()

    pl.run_scoped(phase2, pltpu.VMEM((2, T // (NV // 2), TB), bf16), pltpu.VMEM((2, TB, CN), bf16))

    KE = KD + NH * (NV // 2)
    KL = K0 + OFFS[-1] + PERIOD * (NU - 1) + 1

    def tail(k, c):
        exchange(k)
        return c

    lax.fori_loop(KE, max(KL, KE), tail, 0)
    u = NU - 1
    for d in (0, 1):
        sendA(u, d).wait_send()
        sendB(u, d).wait_send()
        sendC(u, d).wait_send()
        sendG(u, d).wait_send()
        sendR(u, d).wait_send()
        sibG(u, d).wait_send()
    sibO(u).wait_send()
    sibR(u).wait_send()
    ownO(u).wait()

    def sw(u, c):
        sibW(u).wait_recv()
        return c

    lax.fori_loop(0, NU, sw, 0)


def solution(mesh):
    n = mesh.shape['tp']

    def local(X, W, labels):
        T, H = X.shape
        V = W.shape[1]
        NB, NV = T // TB, V // CN
        NU, UR = 2 * NB, TB // 2
        HH = H // 2
        QR = UR // (n // 2)
        HR = QR // 2
        lab = jnp.broadcast_to(labels[:, None], (T, 128))
        f32, bf16 = jnp.float32, jnp.bfloat16
        S = jax.ShapeDtypeStruct
        D = pltpu.SemaphoreType.DMA
        hbm = pl.BlockSpec(memory_space=pl.ANY)
        outs = pl.pallas_call(
            functools.partial(kernel, n),
            out_shape=[S((8, 128), f32), S((H, V), bf16), S((T, H), bf16), S((T, V), bf16), S((T, HH), f32),
                       S((2, NU * HR, HH), f32), S((2, NU * HR, HH), f32), S((2, NU * HR, HH), f32)],
            in_specs=[hbm] * 3,
            out_specs=[pl.BlockSpec(memory_space=pltpu.VMEM)] + [hbm] * 7,
            scratch_shapes=[
                pltpu.VMEM((H, V), bf16), pltpu.VMEM((TB, H), bf16), pltpu.VMEM((TB, V), bf16),
                pltpu.VMEM((HH // CN, TB, CN), f32),
                pltpu.VMEM((2, 8, TB), f32), pltpu.VMEM((2, n, 8, TB), f32),
                pltpu.VMEM((2, HR, HH), f32), pltpu.VMEM((2, HR, HH), f32), pltpu.VMEM((2, HR, HH), f32),
                pltpu.VMEM((2, 2, HR, HH), f32), pltpu.VMEM((QR, HH), bf16),
                D((NV,)), D, D, D((NV,)), D((2, n)), D((2, n)), pltpu.SemaphoreType.REGULAR((HH // CN,)),
                D((2,)), D((HH // CN,)), D((2,)), D((2,)), D((2,)),
                D((2,)), D((2, NU)), D((2,)), D((2, NU)), D((2,)), D((2, NU)), D((2,)), D((2, NU)),
                D((2,)), D((2, NU)), D((4,)), D((NU,)), D((10,)), D,
            ],
            compiler_params=pltpu.CompilerParams(collective_id=0, has_side_effects=True,
                                                 vmem_limit_bytes=67043328),
            cost_estimate=pl.CostEstimate(flops=6 * T * H * V, bytes_accessed=8 * T * H, transcendentals=T * V),
        )(X, W, lab)
        return outs[0][0, :1], outs[1], outs[2]

    return jax.shard_map(local, mesh=mesh,
                         in_specs=(P('dp', None), P(None, 'tp'), P('dp')),
                         out_specs=(P('dp'), P('dp', 'tp'), P('dp', None)),
                         check_vma=False)
```

```python
import functools

import jax
import jax.numpy as jnp
from jax import lax
from jax.experimental import pallas as pl
from jax.experimental.pallas import tpu as pltpu
from jax.sharding import PartitionSpec as P

TB = 512
CN = 512
REST = 2
PERIOD = 5
OFFS = (0, 1, 2, 3, 6, 7, 9, 11)


def kernel(n, X, W, lab, Lo, dW, dX, Gh, Q, rA, rB, rC,
           wg, xb, gb, prs, st_send, st_recv, va, vq, vs, vt, ro,
           wsem, xsem, lsem, gsem, stS, stR, cred, psS, psR, qsem, xssem, odsem,
           aS, aR, bS, bR, cS, cR, gS, gR, rS, rR, sS, sR, ldsem, rosem):
    T, H = X.shape
    V = W.shape[1]
    NB, NV = T // TB, V // CN
    HH = H // 2
    ND = HH // CN
    NU = 2 * NB
    UR = TB // 2
    nc = n // 2
    QR = UR // nc
    HR = QR // 2
    f32, bf16 = jnp.float32, jnp.bfloat16
    me = lax.axis_index('tp')
    core = me % 2
    chip = me // 2
    sib = chip * 2 + 1 - core
    cn, cp, cf = (chip + 1) % nc, (chip + nc - 1) % nc, (chip + 2) % nc
    nxt, prv = cn * 2 + core, cp * 2 + core
    off = me * V

    def rcopy(src, dst, ss, rs, dev):
        return pltpu.make_async_remote_copy(src_ref=src, dst_ref=dst, send_sem=ss, recv_sem=rs,
                                            device_id={'tp': dev}, device_id_type=pl.DeviceIdType.MESH)

    def lcopy(src, dst, sem):
        return pltpu.make_async_copy(src, dst, sem)

    def mo(x, m):
        return x if isinstance(x, int) else pl.multiple_of(x, m)

    def cols(j):
        return pl.ds(mo(j * CN, CN), CN)

    def xcopy(b):
        return lcopy(X.at[pl.ds(mo(b * TB, TB), TB)], xb, xsem)

    def wcopy(j):
        return lcopy(W.at[:, cols(j)], wg.at[:, cols(j)], wsem.at[j])

    def qrows(u, c, h):
        return Q.at[pl.ds(mo(u * UR + c * QR + h * HR, HR), HR)]

    def rrows(r, d, u):
        return r.at[d, pl.ds(mo(u * HR, HR), HR)]

    def xrows(u, c, h, rows, k):
        return dX.at[pl.ds(mo(u * UR + c * QR + h * HR, HR), rows), pl.ds(mo(k * HH, HH), HH)]

    def sendA(u, d):
        return rcopy(qrows(u, cf, d), rrows(rA, d, u), aS.at[d], aR.at[d, u], (nxt, prv)[d])

    def sendB(u, d):
        return rcopy(qrows(u, (cn, cp)[d], 1 - d), rrows(rB, d, u), bS.at[d], bR.at[d, u], (nxt, prv)[d])

    def sendC(u, d):
        return rcopy(va.at[d], rrows(rC, d, u), cS.at[d], cR.at[d, u], (nxt, prv)[d])

    def loadC(u):
        return ([lcopy(rrows(rA, d, u), va.at[d], ldsem.at[d]) for d in (0, 1)]
                + [lcopy(qrows(u, (cn, cp)[d], d), vq.at[d], ldsem.at[2 + d]) for d in (0, 1)])

    def loadS(u):
        return ([lcopy(qrows(u, chip, h), vs.at[h], ldsem.at[4 + h]) for h in (0, 1)]
                + [lcopy(rrows(rC, h, u), vt.at[0, h], ldsem.at[6 + h]) for h in (0, 1)]
                + [lcopy(rrows(rB, 1 - h, u), vt.at[1, h], ldsem.at[8 + h]) for h in (0, 1)])

    def sendG(u, d):
        return rcopy(ro, xrows(u, chip, 0, QR, core), gS.at[d], gR.at[d, u], (nxt, prv)[d])

    def recvG(u, d):
        return rcopy(ro, xrows(u, (cp, cn)[d], 0, QR, core), gS.at[d], gR.at[d, u], (nxt, prv)[d])

    def sendR(u, d):
        r = xrows(u, (cp, cn)[d], d, HR, core)
        return rcopy(r, r, rS.at[d], rR.at[d, u], (nxt, prv)[d])

    def recvR(u, d):
        r = xrows(u, cf, d, HR, core)
        return rcopy(r, r, rS.at[d], rR.at[d, u], (nxt, prv)[d])

    def sibO(u):
        return rcopy(ro, xrows(u, chip, 0, QR, core), sS.at[0], sR.at[u], sib)

    def sibG(u, d):
        r = xrows(u, (cp, cn)[d], 0, QR, core)
        return rcopy(r, r, sS.at[1 + d], sR.at[u], sib)

    def sibR(u):
        r = xrows(u, cf, 0, QR, core)
        return rcopy(r, r, sS.at[3], sR.at[u], sib)

    def sibW(u):
        r = dX.at[pl.ds(mo(u * UR, UR), UR), pl.ds(mo((1 - core) * HH, HH), HH)]
        return rcopy(r, r, sS.at[0], sR.at[u], sib)

    def ownO(u):
        return lcopy(ro, xrows(u, chip, 0, QR, core), rosem)

    def st0(u):
        @pl.when(u > 0)
        def _():
            for d in (0, 1):
                sendA(u - 1, d).wait_send()
        for d in (0, 1):
            sendA(u, d).start()

    def st1(u):
        @pl.when(u > 0)
        def _():
            for d in (0, 1):
                sendB(u - 1, d).wait_send()
        for d in (0, 1):
            sendB(u, d).start()

    def st2(u):
        @pl.when(u > 0)
        def _():
            for d in (0, 1):
                sendC(u - 1, d).wait_send()
        for d in (0, 1):
            sendA(u, d).wait_recv()
        for c in loadC(u):
            c.start()

    def st3(u):
        for c in loadC(u):
            c.wait()
        va[...] = va[...] + vq[...]
        for d in (0, 1):
            sendC(u, d).start()

    def st4(u):
        for d in (0, 1):
            sendB(u, d).wait_recv()
            sendC(u, d).wait_recv()
        for c in loadS(u):
            c.start()

    def st5(u):
        @pl.when(u > 0)
        def _():
            for d in (0, 1):
                sendG(u - 1, d).wait_send()
            sibO(u - 1).wait_send()
            ownO(u - 1).wait()
        for c in loadS(u):
            c.wait()
        for h in (0, 1):
            ro[h * HR:(h + 1) * HR] = ((vt[0, h] + vs[h]) + vt[1, h]).astype(bf16)
        for d in (0, 1):
            sendG(u, d).start()
        ownO(u).start()
        sibO(u).start()

    def st6(u):
        @pl.when(u > 0)
        def _():
            for d in (0, 1):
                sendR(u - 1, d).wait_send()
                sibG(u - 1, d).wait_send()
        for d in (0, 1):
            recvG(u, d).wait_recv()
        for d in (0, 1):
            sendR(u, d).start()
        for d in (0, 1):
            sibG(u, d).start()

    def st7(u):
        @pl.when(u > 0)
        def _():
            sibR(u - 1).wait_send()
        for d in (0, 1):
            recvR(u, d).wait_recv()
        sibR(u).start()

    ST = NV // 2
    K0 = 3 * ST

    def exchange(k):
        for o, fn in reversed(tuple(zip(OFFS, (st0, st1, st2, st3, st4, st5, st6, st7)))):
            t = k - (K0 + o)
            u = t // PERIOD

            @pl.when((t >= 0) & (t % PERIOD == 0) & (u < NU))
            def _(fn=fn, u=u):
                fn(u)

    barrier = pltpu.get_barrier_semaphore()
    for i in range(1, n):
        pl.semaphore_signal(barrier, inc=1, device_id={'tp': (me + i) % n}, device_id_type=pl.DeviceIdType.MESH)
    pl.semaphore_wait(barrier, n - 1)
    xcopy(0).start()
    for j in range(NV):
        wcopy(j).start()

    def stat_copy(par, i):
        peer = (me + i) % n
        return rcopy(st_send.at[par], st_recv.at[par, me], stS.at[par, i], stR.at[par, me], peer)

    def stat_recv(par, i):
        src = (me + n - i) % n
        return rcopy(st_send.at[par], st_recv.at[par, src], stS.at[par, i], stR.at[par, src], src)

    def gcopy(b):
        return lcopy(gb, Gh.at[pl.ds(mo(b * TB, TB), TB)], gsem.at[0])

    def phase1(eb, za, zb, ps, qs, lb, m_run, s_run, z_run, mjs, lacc):
        RT = min(64, TB)
        lane = lax.broadcasted_iota(jnp.int32, (RT, 128), 1)
        laneT = lax.broadcasted_iota(jnp.int32, (TB, 128), 1)

        def lcp(b):
            return lcopy(lab.at[pl.ds(mo(b * TB, TB), TB)], lb.at[b % 2], lsem)

        lcp(0).start()
        lacc[...] = jnp.zeros_like(lacc)

        def zdot(j, z):
            z[...] = jnp.dot(xb[...], wg[:, cols(j)], preferred_element_type=f32)

        def epi(z, j, par):
            base = j * CN
            for r in range(0, TB, RT):
                rows = slice(r, r + RT)
                zq = [z[rows, q * 128:(q + 1) * 128] for q in range(CN // 128)]
                mx = functools.reduce(jnp.maximum, zq)
                m_old = m_run[rows]
                m_new = jnp.maximum(m_old, jnp.max(mx, axis=1, keepdims=True))
                m_run[rows] = m_new
                mjs[rows] = jnp.where(lane == j, m_new, mjs[rows])
                s = s_run[rows] * jnp.exp(m_old - m_new)
                t = z_run[rows]
                lb_r = lb[par, rows] - (off + base)
                for q in range(CN // 128):
                    e = jnp.exp(zq[q] - m_new)
                    eb[j, rows, q * 128:(q + 1) * 128] = e
                    s = s + e
                    t = t + jnp.where(lane + q * 128 == lb_r, zq[q], 0.0)
                s_run[rows] = s
                z_run[rows] = t

        def zphase(b):
            par = b % 2
            xcopy(b).wait()
            lcp(b).wait()
            m_run[...] = jnp.full_like(m_run, -jnp.inf)
            s_run[...] = jnp.zeros_like(s_run)
            z_run[...] = jnp.zeros_like(z_run)
            mjs[...] = jnp.zeros_like(mjs)

            def wwait(j):
                @pl.when(b == 0)
                def _():
                    wcopy(j).wait()

            wwait(0)
            zdot(0, za)

            def body(i, c):
                exchange(2 * ST * b - ST + i)
                wwait(2 * i + 1)
                wwait(2 * i + 2)
                zdot(2 * i + 1, zb)
                epi(za, 2 * i, par)
                zdot(2 * i + 2, za)
                epi(zb, 2 * i + 1, par)
                return c

            lax.fori_loop(0, NV // 2 - 1, body, 0)
            exchange(2 * ST * b - 1)
            wwait(NV - 1)
            zdot(NV - 1, zb)
            epi(za, NV - 2, par)

            @pl.when(b < NB - 1)
            def _():
                xcopy(b + 1).start()
            epi(zb, NV - 1, par)

        def send_stats(b):
            par = b % 2
            s = jnp.sum(s_run[...], axis=1, keepdims=True)
            t = jnp.sum(z_run[...], axis=1, keepdims=True)
            a = jnp.where(laneT == 0, m_run[...], jnp.where(laneT == 1, s, jnp.where(laneT == 2, t, 0.0)))
            at = a.T[0:8]

            @pl.when(b >= 2)
            def _():
                for i in range(1, n):
                    stat_copy(par, i).wait_send()
            st_send[par] = at
            st_recv[par, me] = at
            for i in range(1, n):
                stat_copy(par, i).start()

        def gpass(b):
            par = b % 2
            for i in range(1, n):
                stat_recv(par, i).wait_recv()
            ms = [st_recv[par, i, 0:1] for i in range(n)]
            M = functools.reduce(jnp.maximum, ms)
            S = sum(st_recv[par, i, 1:2] * jnp.exp(ms[i] - M) for i in range(n))
            zt = sum(st_recv[par, i, 2:3] for i in range(n))
            lacc[...] = lacc[...] + ((M + jnp.log(S)) - zt)
            sub = lax.broadcasted_iota(jnp.int32, (128, TB), 0)
            bt = jnp.where(sub == 0, M, jnp.where(sub == 1, 1.0 / S, 0.0)).T
            R = jnp.exp(mjs[...] - bt[:, 0:1]) * bt[:, 1:2]
            mjs[...] = R

            @pl.when(b > 0)
            def _():
                gcopy(b - 1).wait()

            def body(j, c):
                for r in range(0, TB, RT):
                    rows = slice(r, r + RT)
                    rj = jnp.sum(jnp.where(lane == j, mjs[rows], 0.0), axis=1, keepdims=True)
                    lb_r = lb[par, rows] - (off + j * CN)
                    for q in range(CN // 128):
                        e = eb[j, rows, q * 128:(q + 1) * 128] * rj
                        e = (e - jnp.where(lane + q * 128 == lb_r, 1.0, 0.0)) * (1.0 / T)
                        gb[rows, pl.ds(mo(j * CN + q * 128, 128), 128)] = e.astype(bf16)
                return c

            lax.fori_loop(0, NV, body, 0)
            gcopy(b).start()

        def dxdot(row0):
            return lax.dot_general(gb[...], wg[pl.ds(mo(row0, CN), CN), :], (((1,), (1,)), ((), ())),
                                   preferred_element_type=f32)

        def pscopy(j, s):
            return rcopy(ps.at[s], prs.at[j], psS.at[s], psR.at[j], sib)

        def qcopy(b, j, s):
            return lcopy(qs.at[s], Q.at[pl.ds(mo(b * TB, TB), TB), cols(j)], qsem.at[s])

        def dxphase(b, k0):
            def body_s(i, c):
                exchange(k0 + i)

                @pl.when(i > 0)
                def _():
                    for s in (0, 1):
                        pscopy(2 * i - 2 + s, s).wait_send()

                @pl.when(b > 0)
                def _():
                    for s in (0, 1):
                        pl.semaphore_wait(cred.at[2 * i + s], 1)
                for s in (0, 1):
                    ps[s] = dxdot((1 - core) * HH + (2 * i + s) * CN)
                for s in (0, 1):
                    pscopy(2 * i + s, s).start()
                return c

            lax.fori_loop(0, ND // 2, body_s, 0)

            def body_o(i, c):
                exchange(k0 + ND // 2 + i)

                @pl.when(i > 0)
                def _():
                    for s in (0, 1):
                        qcopy(b, 2 * i - 2 + s, s).wait()
                for s in (0, 1):
                    pscopy(2 * i + s, s).wait_recv()
                for s in (0, 1):
                    qs[s] = dxdot(core * HH + (2 * i + s) * CN) + prs[2 * i + s]
                for s in (0, 1):
                    qcopy(b, 2 * i + s, s).start()

                @pl.when(b < NB - 1)
                def _():
                    for s in (0, 1):
                        pl.semaphore_signal(cred.at[2 * i + s], inc=1, device_id={'tp': sib},
                                            device_id_type=pl.DeviceIdType.MESH)
                return c

            lax.fori_loop(0, ND // 2, body_o, 0)
            for s in (0, 1):
                pscopy(ND - 2 + s, s).wait_send()

        def block(b, c):
            @pl.when(b < NB)
            def _():
                zphase(b)
                send_stats(b)

                @pl.when(b < NB - 1)
                def _():
                    lcp(b + 1).start()

            @pl.when(b == NB)
            def _():
                for i in range(T // TB):
                    x0copy(i).start()

            @pl.when(b > 0)
            def _():
                dxphase(b - 1, jnp.minimum(2 * ST * b, (2 * NB - 1) * ST))

            @pl.when(b < NB)
            def _():
                gpass(b)

            @pl.when(b > 0)
            def _():
                for s in (0, 1):
                    qcopy(b - 1, ND - 2 + s, s).wait()
            return c

        lax.fori_loop(0, NB + 1, block, 0)
        for b in (NB - 2, NB - 1):
            for i in range(1, n):
                stat_copy(b % 2, i).wait_send()
        Lo[...] = jnp.zeros_like(Lo) + jnp.sum(lacc[...], axis=1, keepdims=True) * (1.0 / T)

    def x0copy(i):
        return lcopy(X.at[pl.ds(i * TB, TB), pl.ds(0, TB)], xb.at[:, pl.ds(i * TB, TB)], wsem.at[i])

    pl.run_scoped(phase1,
                  pltpu.VMEM((NV, TB, CN), f32), pltpu.VMEM((TB, CN), f32), pltpu.VMEM((TB, CN), f32),
                  pltpu.VMEM((2, TB, CN), f32), pltpu.VMEM((2, TB, CN), f32), pltpu.VMEM((2, TB, 128), jnp.int32),
                  pltpu.VMEM((TB, 128), f32), pltpu.VMEM((TB, 128), f32), pltpu.VMEM((TB, 128), f32),
                  pltpu.VMEM((TB, 128), f32), pltpu.VMEM((1, TB), f32))

    KD = 2 * ST * NB
    NH = H // TB - REST

    def phase2(xs, od):
        SL = T // (NV // 2)

        def gload(j):
            return lcopy(Gh.at[:, cols(j)], wg.at[:, cols(j)], gsem.at[j])

        def xscopy(h, i):
            return lcopy(X.at[pl.ds(mo(i * SL, SL), SL), pl.ds(mo(h * TB, TB), TB)], xs.at[i % 2], xssem.at[i % 2])

        def odcopy(h, j, s):
            return lcopy(od.at[s], dW.at[pl.ds(mo(h * TB, TB), TB), cols(j)], odsem.at[s])

        gcopy(NB - 1).wait()
        for j in range(NV):
            gload(j).start()
        xscopy(1, 0).start()
        for i in range(T // TB):
            x0copy(i).wait()

        def tr0(i, c):
            gb[:, pl.ds(mo(i * TB, TB), TB)] = xb[:, pl.ds(mo(i * TB, TB), TB)].T
            return c

        lax.fori_loop(0, T // TB, tr0, 0)

        def hstep(h, cur, fut):
            def body(i, c):
                exchange(KD + h * (NV // 2) + i)

                @pl.when(h == 0)
                def _():
                    gload(2 * i).wait()
                    gload(2 * i + 1).wait()

                @pl.when((h > 0) | (i > 0))
                def _():
                    for s in (0, 1):
                        odcopy(h, 2 * i + s, s).wait()
                hn = jnp.minimum(h + 1, NH - 1)
                xscopy(hn, i).wait()

                @pl.when((h < NH - 1) | (i < NV // 2 - 1))
                def _():
                    last = i == NV // 2 - 1
                    xscopy(jnp.minimum(jnp.where(last, h + 2, h + 1), NH - 1), jnp.where(last, 0, i + 1)).start()
                for s in (0, 1):
                    od[s] = jnp.dot(cur[...], wg[:, cols(2 * i + s)], preferred_element_type=f32).astype(bf16)
                fut[:, pl.ds(mo(i * SL, SL), SL)] = xs[i % 2].T
                for s in (0, 1):
                    odcopy(h, 2 * i + s, s).start()
                return c

            lax.fori_loop(0, NV // 2, body, 0)

        def hpair(hh, c):
            hstep(2 * hh, gb, xb)
            hstep(2 * hh + 1, xb, gb)
            return c

        lax.fori_loop(0, NH // 2, hpair, 0)
        for s in (0, 1):
            odcopy(NH - 1, NV - 2 + s, s).wait()

    pl.run_scoped(phase2, pltpu.VMEM((2, T // (NV // 2), TB), bf16), pltpu.VMEM((2, TB, CN), bf16))

    KE = KD + NH * (NV // 2)
    KL = K0 + OFFS[-1] + PERIOD * (NU - 1) + 1

    def tail(k, c):
        exchange(k)
        return c

    lax.fori_loop(KE, max(KL, KE), tail, 0)
    u = NU - 1
    for d in (0, 1):
        sendA(u, d).wait_send()
        sendB(u, d).wait_send()
        sendC(u, d).wait_send()
        sendG(u, d).wait_send()
        sendR(u, d).wait_send()
        sibG(u, d).wait_send()
    sibO(u).wait_send()
    sibR(u).wait_send()
    ownO(u).wait()

    def sw(u, c):
        sibW(u).wait_recv()
        return c

    lax.fori_loop(0, NU, sw, 0)


def rest(X, Gh, dWa, dXa, dW, dXo, wg, xa, xb, xs, od, cx, cw, gsem, x0sem, xssem, odsem, cxsem, cwsem):
    T, H = X.shape
    V = Gh.shape[1]
    NV = V // CN
    ST = NV // 2
    NH = H // TB
    H0 = NH - REST
    SL = T // ST
    NS = REST * ST
    f32, bf16 = jnp.float32, jnp.bfloat16
    mo = pl.multiple_of
    RX, RW = T // NS, H0 * TB // NS

    def lcopy(src, dst, sem):
        return pltpu.make_async_copy(src, dst, sem)

    def cols(j):
        return pl.ds(mo(j * CN, CN), CN)

    def gload(j):
        return lcopy(Gh.at[:, cols(j)], wg.at[:, cols(j)], gsem.at[j])

    def x0copy(i):
        return lcopy(X.at[pl.ds(i * TB, TB), pl.ds(H0 * TB, TB)], xb.at[:, pl.ds(i * TB, TB)], x0sem.at[i])

    def xscopy(h, i):
        return lcopy(X.at[pl.ds(mo(i * SL, SL), SL), pl.ds(mo(h * TB, TB), TB)], xs.at[i % 2], xssem.at[i % 2])

    def odcopy(h, j, s):
        return lcopy(od.at[s], dW.at[pl.ds(h * TB, TB), cols(j)], odsem.at[s])

    def cin(c):
        return (lcopy(dXa.at[pl.ds(mo(c * RX, RX), RX)], cx.at[c % 2], cxsem.at[0, c % 2]),
                lcopy(dWa.at[pl.ds(mo(c * RW, RW), RW)], cw.at[c % 2], cwsem.at[0, c % 2]))

    def cout(c):
        return (lcopy(cx.at[c % 2], dXo.at[pl.ds(mo(c * RX, RX), RX)], cxsem.at[1, c % 2]),
                lcopy(cw.at[c % 2], dW.at[pl.ds(mo(c * RW, RW), RW)], cwsem.at[1, c % 2]))

    for i in range(T // TB):
        x0copy(i).start()
    for j in (0, 1):
        gload(j).start()
    xscopy(H0 + 1, 0).start()
    for x in cin(0):
        x.start()
    for j in range(2, NV):
        gload(j).start()
    for i in range(T // TB):
        x0copy(i).wait()

    def tr0(i, c):
        xa[:, pl.ds(mo(i * TB, TB), TB)] = xb[:, pl.ds(mo(i * TB, TB), TB)].T
        return c

    lax.fori_loop(0, T // TB, tr0, 0)

    def hstep(r, cur, fut):
        h = H0 + r

        def body(i, c):
            q = r * ST + i

            @pl.when(q > 0)
            def _():
                for x in cout(q - 1):
                    x.wait()

            @pl.when(q < NS - 1)
            def _():
                for x in cin(q + 1):
                    x.start()
            for x in cin(q):
                x.wait()
            for x in cout(q):
                x.start()
            if r == 0:
                gload(2 * i).wait()
                gload(2 * i + 1).wait()
            if r < REST - 1:
                xscopy(h + 1, i).wait()

                @pl.when((i < ST - 1) | (r < REST - 2))
                def _():
                    last = i == ST - 1
                    xscopy(jnp.where(last, h + 2, h + 1), jnp.where(last, 0, i + 1)).start()

            @pl.when(q > 0)
            def _():
                for s in (0, 1):
                    odcopy(h, 2 * i + s, s).wait()
            for s in (0, 1):
                od[s] = jnp.dot(cur[...], wg[:, cols(2 * i + s)], preferred_element_type=f32).astype(bf16)
            if r < REST - 1:
                fut[:, pl.ds(mo(i * SL, SL), SL)] = xs[i % 2].T
            for s in (0, 1):
                odcopy(h, 2 * i + s, s).start()
            return c

        lax.fori_loop(0, ST, body, 0)

    for r in range(REST):
        hstep(r, (xa, xb)[r % 2], (xb, xa)[r % 2])
    for s in (0, 1):
        odcopy(NH - 1, NV - 2 + s, s).wait()
    for x in cout(NS - 1):
        x.wait()


def solution(mesh):
    n = mesh.shape['tp']

    def local(X, W, labels):
        T, H = X.shape
        V = W.shape[1]
        NB, NV = T // TB, V // CN
        NU, UR = 2 * NB, TB // 2
        HH = H // 2
        QR = UR // (n // 2)
        HR = QR // 2
        lab = jnp.broadcast_to(labels[:, None], (T, 128))
        f32, bf16 = jnp.float32, jnp.bfloat16
        S = jax.ShapeDtypeStruct
        D = pltpu.SemaphoreType.DMA
        hbm = pl.BlockSpec(memory_space=pl.ANY)
        outs = pl.pallas_call(
            functools.partial(kernel, n),
            out_shape=[S((8, 128), f32), S((H - REST * TB, V), bf16), S((T, H), bf16), S((T, V), bf16), S((T, HH), f32),
                       S((2, NU * HR, HH), f32), S((2, NU * HR, HH), f32), S((2, NU * HR, HH), f32)],
            in_specs=[hbm] * 3,
            out_specs=[pl.BlockSpec(memory_space=pltpu.VMEM)] + [hbm] * 7,
            scratch_shapes=[
                pltpu.VMEM((H, V), bf16), pltpu.VMEM((TB, H), bf16), pltpu.VMEM((TB, V), bf16),
                pltpu.VMEM((HH // CN, TB, CN), f32),
                pltpu.VMEM((2, 8, TB), f32), pltpu.VMEM((2, n, 8, TB), f32),
                pltpu.VMEM((2, HR, HH), f32), pltpu.VMEM((2, HR, HH), f32), pltpu.VMEM((2, HR, HH), f32),
                pltpu.VMEM((2, 2, HR, HH), f32), pltpu.VMEM((QR, HH), bf16),
                D((NV,)), D, D, D((NV,)), D((2, n)), D((2, n)), pltpu.SemaphoreType.REGULAR((HH // CN,)),
                D((2,)), D((HH // CN,)), D((2,)), D((2,)), D((2,)),
                D((2,)), D((2, NU)), D((2,)), D((2, NU)), D((2,)), D((2, NU)), D((2,)), D((2, NU)),
                D((2,)), D((2, NU)), D((4,)), D((NU,)), D((10,)), D,
            ],
            compiler_params=pltpu.CompilerParams(collective_id=0, has_side_effects=True,
                                                 vmem_limit_bytes=67043328),
            cost_estimate=pl.CostEstimate(flops=6 * T * H * V, bytes_accessed=8 * T * H, transcendentals=T * V),
        )(X, W, lab)
        ST = NV // 2
        NS = REST * ST
        dW, dX = pl.pallas_call(
            rest,
            out_shape=[S((H, V), bf16), S((T, H), bf16)],
            in_specs=[hbm] * 4,
            out_specs=[hbm] * 2,
            scratch_shapes=[
                pltpu.VMEM((T, V), bf16), pltpu.VMEM((TB, T), bf16), pltpu.VMEM((TB, T), bf16),
                pltpu.VMEM((2, T // ST, TB), bf16), pltpu.VMEM((2, TB, CN), bf16),
                pltpu.VMEM((2, T // NS, H), bf16), pltpu.VMEM((2, (H - REST * TB) // NS, V), bf16),
                D((NV,)), D((T // TB,)), D((2,)), D((2,)), D((2, 2)), D((2, 2)),
            ],
            compiler_params=pltpu.CompilerParams(vmem_limit_bytes=67043328),
            cost_estimate=pl.CostEstimate(flops=2 * T * REST * TB * V, bytes_accessed=10 * T * H, transcendentals=0),
        )(X, outs[3], outs[1], outs[2])
        return outs[0][0, :1], dW, dX

    return jax.shard_map(local, mesh=mesh,
                         in_specs=(P('dp', None), P(None, 'tp'), P('dp')),
                         out_specs=(P('dp'), P('dp', 'tp'), P('dp', None)),
                         check_vma=False)
```

```python
import functools

import jax
import jax.numpy as jnp
from jax import lax
from jax.experimental import pallas as pl
from jax.experimental.pallas import tpu as pltpu
from jax.sharding import PartitionSpec as P

PAIR = tuple(range(2))
TB = 512
CN = 512
REST = 2
PERIOD = 5
OFFS = (0, 1, 2, 3, 6, 7, 9, 11)


def kernel(n, X, W, lab, Lo, dW, dX, Gh, Q, rA, rB, rC,
           wg, xb, gb, prs, st_send, st_recv, va, vq, vs, vt, ro,
           wsem, xsem, lsem, gsem, stS, stR, cred, psS, psR, qsem, xssem, odsem,
           aS, aR, bS, bR, cS, cR, gS, gR, rS, rR, sS, sR, ldsem, rosem):
    T, H = X.shape
    V = W.shape[1]
    NB, NV = T // TB, V // CN
    HH = H // 2
    ND = HH // CN
    NU = 2 * NB
    UR = TB // 2
    nc = n // 2
    QR = UR // nc
    HR = QR // 2
    f32, bf16 = jnp.float32, jnp.bfloat16
    me = lax.axis_index('tp')
    core = me % 2
    chip = me // 2
    sib = chip * 2 + 1 - core
    cn, cp, cf = (chip + 1) % nc, (chip + nc - 1) % nc, (chip + 2) % nc
    nxt, prv = cn * 2 + core, cp * 2 + core
    off = me * V

    def rcopy(src, dst, ss, rs, dev):
        return pltpu.make_async_remote_copy(src_ref=src, dst_ref=dst, send_sem=ss, recv_sem=rs,
                                            device_id={'tp': dev}, device_id_type=pl.DeviceIdType.MESH)

    def lcopy(src, dst, sem):
        return pltpu.make_async_copy(src, dst, sem)

    def mo(x, m):
        return x if isinstance(x, int) else pl.multiple_of(x, m)

    def cols(j):
        return pl.ds(mo(j * CN, CN), CN)

    def xcopy(b):
        return lcopy(X.at[pl.ds(mo(b * TB, TB), TB)], xb, xsem)

    def wcopy(j):
        return lcopy(W.at[:, cols(j)], wg.at[:, cols(j)], wsem.at[j])

    def qrows(u, c, h):
        return Q.at[pl.ds(mo(u * UR + c * QR + h * HR, HR), HR)]

    def rrows(r, d, u):
        return r.at[d, pl.ds(mo(u * HR, HR), HR)]

    def xrows(u, c, h, rows, k):
        return dX.at[pl.ds(mo(u * UR + c * QR + h * HR, HR), rows), pl.ds(mo(k * HH, HH), HH)]

    def sendA(u, d):
        return rcopy(qrows(u, cf, d), rrows(rA, d, u), aS.at[d], aR.at[d, u], (nxt, prv)[d])

    def sendB(u, d):
        return rcopy(qrows(u, (cn, cp)[d], 1 - d), rrows(rB, d, u), bS.at[d], bR.at[d, u], (nxt, prv)[d])

    def sendC(u, d):
        return rcopy(va.at[d], rrows(rC, d, u), cS.at[d], cR.at[d, u], (nxt, prv)[d])

    def loadC(u):
        return ([lcopy(rrows(rA, d, u), va.at[d], ldsem.at[d]) for d in PAIR]
                + [lcopy(qrows(u, (cn, cp)[d], d), vq.at[d], ldsem.at[2 + d]) for d in PAIR])

    def loadS(u):
        return ([lcopy(qrows(u, chip, h), vs.at[h], ldsem.at[4 + h]) for h in PAIR]
                + [lcopy(rrows(rC, h, u), vt.at[0, h], ldsem.at[6 + h]) for h in PAIR]
                + [lcopy(rrows(rB, 1 - h, u), vt.at[1, h], ldsem.at[8 + h]) for h in PAIR])

    def sendG(u, d):
        return rcopy(ro, xrows(u, chip, 0, QR, core), gS.at[d], gR.at[d, u], (nxt, prv)[d])

    def recvG(u, d):
        return rcopy(ro, xrows(u, (cp, cn)[d], 0, QR, core), gS.at[d], gR.at[d, u], (nxt, prv)[d])

    def sendR(u, d):
        r = xrows(u, (cp, cn)[d], d, HR, core)
        return rcopy(r, r, rS.at[d], rR.at[d, u], (nxt, prv)[d])

    def recvR(u, d):
        r = xrows(u, cf, d, HR, core)
        return rcopy(r, r, rS.at[d], rR.at[d, u], (nxt, prv)[d])

    def sibO(u):
        return rcopy(ro, xrows(u, chip, 0, QR, core), sS.at[0], sR.at[u], sib)

    def sibG(u, d):
        r = xrows(u, (cp, cn)[d], 0, QR, core)
        return rcopy(r, r, sS.at[1 + d], sR.at[u], sib)

    def sibR(u):
        r = xrows(u, cf, 0, QR, core)
        return rcopy(r, r, sS.at[3], sR.at[u], sib)

    def sibW(u):
        r = dX.at[pl.ds(mo(u * UR, UR), UR), pl.ds(mo((1 - core) * HH, HH), HH)]
        return rcopy(r, r, sS.at[0], sR.at[u], sib)

    def ownO(u):
        return lcopy(ro, xrows(u, chip, 0, QR, core), rosem)

    def st0(u):
        @pl.when(u > 0)
        def _():
            for d in PAIR:
                sendA(u - 1, d).wait_send()
        for d in PAIR:
            sendA(u, d).start()

    def st1(u):
        @pl.when(u > 0)
        def _():
            for d in PAIR:
                sendB(u - 1, d).wait_send()
        for d in PAIR:
            sendB(u, d).start()

    def st2(u):
        @pl.when(u > 0)
        def _():
            for d in PAIR:
                sendC(u - 1, d).wait_send()
        for d in PAIR:
            sendA(u, d).wait_recv()
        for c in loadC(u):
            c.start()

    def st3(u):
        for c in loadC(u):
            c.wait()
        va[...] = va[...] + vq[...]
        for d in PAIR:
            sendC(u, d).start()

    def st4(u):
        for d in PAIR:
            sendB(u, d).wait_recv()
            sendC(u, d).wait_recv()
        for c in loadS(u):
            c.start()

    def st5(u):
        @pl.when(u > 0)
        def _():
            for d in PAIR:
                sendG(u - 1, d).wait_send()
            sibO(u - 1).wait_send()
            ownO(u - 1).wait()
        for c in loadS(u):
            c.wait()
        for h in PAIR:
            ro[h * HR:(h + 1) * HR] = ((vt[0, h] + vs[h]) + vt[1, h]).astype(bf16)
        for d in PAIR:
            sendG(u, d).start()
        ownO(u).start()
        sibO(u).start()

    def st6(u):
        @pl.when(u > 0)
        def _():
            for d in PAIR:
                sendR(u - 1, d).wait_send()
                sibG(u - 1, d).wait_send()
        for d in PAIR:
            recvG(u, d).wait_recv()
        for d in PAIR:
            sendR(u, d).start()
        for d in PAIR:
            sibG(u, d).start()

    def st7(u):
        @pl.when(u > 0)
        def _():
            sibR(u - 1).wait_send()
        for d in PAIR:
            recvR(u, d).wait_recv()
        sibR(u).start()

    ST = NV // 2
    K0 = 3 * ST

    def exchange(k):
        t = jnp.asarray(k + K0 * PERIOD - K0, jnp.int32)
        q, r = lax.div(t, PERIOD) - K0, lax.rem(t, PERIOD)
        for o, fn in reversed(tuple(zip(OFFS, (st0, st1, st2, st3, st4, st5, st6, st7)))):
            u = q - o // PERIOD

            @pl.when((r == o % PERIOD) & (u >= 0) & (u < NU))
            def _(fn=fn, u=u):
                fn(u)

    barrier = pltpu.get_barrier_semaphore()
    for i in range(1, n):
        pl.semaphore_signal(barrier, inc=1, device_id={'tp': (me + i) % n}, device_id_type=pl.DeviceIdType.MESH)
    pl.semaphore_wait(barrier, n - 1)
    xcopy(0).start()
    for j in range(NV):
        wcopy(j).start()

    def stat_copy(par, i):
        peer = (me + i) % n
        return rcopy(st_send.at[par], st_recv.at[par, me], stS.at[par, i], stR.at[par, me], peer)

    def stat_recv(par, i):
        src = (me + n - i) % n
        return rcopy(st_send.at[par], st_recv.at[par, src], stS.at[par, i], stR.at[par, src], src)

    def gcopy(b):
        return lcopy(gb, Gh.at[pl.ds(mo(b * TB, TB), TB)], gsem.at[0])

    def phase1(eb, za, zb, ps, qs, lb, m_run, s_run, z_run, mjs, lacc):
        RT = min(64, TB)
        lane = lax.broadcasted_iota(jnp.int32, (RT, 128), 1)
        laneT = lax.broadcasted_iota(jnp.int32, (TB, 128), 1)

        def lcp(b):
            return lcopy(lab.at[pl.ds(mo(b * TB, TB), TB)], lb.at[b % 2], lsem)

        lcp(0).start()
        lacc[...] = jnp.zeros_like(lacc)

        def zdot(j, z):
            z[...] = jnp.dot(xb[...], wg[:, cols(j)], preferred_element_type=f32)

        def epi(z, j, par):
            base = j * CN
            for r in range(0, TB, RT):
                rows = slice(r, r + RT)
                zq = [z[rows, q * 128:(q + 1) * 128] for q in range(CN // 128)]
                mx = functools.reduce(jnp.maximum, zq)
                m_old = m_run[rows]
                m_new = jnp.maximum(m_old, jnp.max(mx, axis=1, keepdims=True))
                m_run[rows] = m_new
                mjs[rows] = jnp.where(lane == j, m_new, mjs[rows])
                s = s_run[rows] * jnp.exp(m_old - m_new)
                t = z_run[rows]
                lb_r = lb[par, rows] - (off + base)
                for q in range(CN // 128):
                    e = jnp.exp(zq[q] - m_new)
                    eb[j, rows, q * 128:(q + 1) * 128] = e
                    s = s + e
                    t = t + jnp.where(lane + q * 128 == lb_r, zq[q], 0.0)
                s_run[rows] = s
                z_run[rows] = t

        def zphase(b):
            par = b % 2
            xcopy(b).wait()
            lcp(b).wait()
            m_run[...] = jnp.full_like(m_run, -jnp.inf)
            s_run[...] = jnp.zeros_like(s_run)
            z_run[...] = jnp.zeros_like(z_run)
            mjs[...] = jnp.zeros_like(mjs)

            def wwait(j):
                @pl.when(b == 0)
                def _():
                    wcopy(j).wait()

            wwait(0)
            zdot(0, za)

            def body(i, c):
                exchange(2 * ST * b - ST + i)
                wwait(2 * i + 1)
                wwait(2 * i + 2)
                zdot(2 * i + 1, zb)
                epi(za, 2 * i, par)
                zdot(2 * i + 2, za)
                epi(zb, 2 * i + 1, par)
                return c

            lax.fori_loop(0, NV // 2 - 1, body, 0)
            exchange(2 * ST * b - 1)
            wwait(NV - 1)
            zdot(NV - 1, zb)
            epi(za, NV - 2, par)

            @pl.when(b < NB - 1)
            def _():
                xcopy(b + 1).start()
            epi(zb, NV - 1, par)

        def send_stats(b):
            par = b % 2
            s = jnp.sum(s_run[...], axis=1, keepdims=True)
            t = jnp.sum(z_run[...], axis=1, keepdims=True)
            a = jnp.where(laneT == 0, m_run[...], jnp.where(laneT == 1, s, jnp.where(laneT == 2, t, 0.0)))
            at = a.T[0:8]

            @pl.when(b >= 2)
            def _():
                for i in range(1, n):
                    stat_copy(par, i).wait_send()
            st_send[par] = at
            st_recv[par, me] = at
            for i in range(1, n):
                stat_copy(par, i).start()

        def gpass(b):
            par = b % 2
            for i in range(1, n):
                stat_recv(par, i).wait_recv()
            ms = [st_recv[par, i, 0:1] for i in range(n)]
            M = functools.reduce(jnp.maximum, ms)
            S = sum(st_recv[par, i, 1:2] * jnp.exp(ms[i] - M) for i in range(n))
            zt = sum(st_recv[par, i, 2:3] for i in range(n))
            lacc[...] = lacc[...] + ((M + jnp.log(S)) - zt)
            sub = lax.broadcasted_iota(jnp.int32, (128, TB), 0)
            bt = jnp.where(sub == 0, M, jnp.where(sub == 1, 1.0 / S, 0.0)).T
            R = jnp.exp(mjs[...] - bt[:, 0:1]) * bt[:, 1:2]
            mjs[...] = R

            @pl.when(b > 0)
            def _():
                gcopy(b - 1).wait()

            def body(j, c):
                for r in range(0, TB, RT):
                    rows = slice(r, r + RT)
                    rj = jnp.sum(jnp.where(lane == j, mjs[rows], 0.0), axis=1, keepdims=True)
                    lb_r = lb[par, rows] - (off + j * CN)
                    for q in range(CN // 128):
                        e = eb[j, rows, q * 128:(q + 1) * 128] * rj
                        e = (e - jnp.where(lane + q * 128 == lb_r, 1.0, 0.0)) * (1.0 / T)
                        gb[rows, pl.ds(mo(j * CN + q * 128, 128), 128)] = e.astype(bf16)
                return c

            lax.fori_loop(0, NV, body, 0)
            gcopy(b).start()

        def dxdot(row0):
            return lax.dot_general(gb[...], wg[pl.ds(mo(row0, CN), CN), :], (((1,), (1,)), ((), ())),
                                   preferred_element_type=f32)

        def pscopy(j, s):
            return rcopy(ps.at[s], prs.at[j], psS.at[s], psR.at[j], sib)

        def qcopy(b, j, s):
            return lcopy(qs.at[s], Q.at[pl.ds(mo(b * TB, TB), TB), cols(j)], qsem.at[s])

        def dxphase(b, k0):
            def body_s(i, c):
                exchange(k0 + i)

                @pl.when(i > 0)
                def _():
                    for s in PAIR:
                        pscopy(2 * i - 2 + s, s).wait_send()

                @pl.when(b > 0)
                def _():
                    for s in PAIR:
                        pl.semaphore_wait(cred.at[2 * i + s], 1)
                for s in PAIR:
                    ps[s] = dxdot((1 - core) * HH + (2 * i + s) * CN)
                for s in PAIR:
                    pscopy(2 * i + s, s).start()
                return c

            lax.fori_loop(0, ND // 2, body_s, 0)

            def body_o(i, c):
                exchange(k0 + ND // 2 + i)

                @pl.when(i > 0)
                def _():
                    for s in PAIR:
                        qcopy(b, 2 * i - 2 + s, s).wait()
                for s in PAIR:
                    pscopy(2 * i + s, s).wait_recv()
                for s in PAIR:
                    qs[s] = dxdot(core * HH + (2 * i + s) * CN) + prs[2 * i + s]
                for s in PAIR:
                    qcopy(b, 2 * i + s, s).start()

                @pl.when(b < NB - 1)
                def _():
                    for s in PAIR:
                        pl.semaphore_signal(cred.at[2 * i + s], inc=1, device_id={'tp': sib},
                                            device_id_type=pl.DeviceIdType.MESH)
                return c

            lax.fori_loop(0, ND // 2, body_o, 0)
            for s in PAIR:
                pscopy(ND - 2 + s, s).wait_send()

        def block(b, c):
            @pl.when(b < NB)
            def _():
                zphase(b)
                send_stats(b)

                @pl.when(b < NB - 1)
                def _():
                    lcp(b + 1).start()

            @pl.when(b == NB)
            def _():
                for i in range(T // TB):
                    x0copy(i).start()

            @pl.when(b > 0)
            def _():
                dxphase(b - 1, jnp.minimum(2 * ST * b, (2 * NB - 1) * ST))

            @pl.when(b < NB)
            def _():
                gpass(b)

            @pl.when(b > 0)
            def _():
                for s in PAIR:
                    qcopy(b - 1, ND - 2 + s, s).wait()
            return c

        lax.fori_loop(0, NB + 1, block, 0)
        for b in (NB - 2, NB - 1):
            for i in range(1, n):
                stat_copy(b % 2, i).wait_send()
        Lo[...] = jnp.zeros_like(Lo) + jnp.sum(lacc[...], axis=1, keepdims=True) * (1.0 / T)

    def x0copy(i):
        return lcopy(X.at[pl.ds(i * TB, TB), pl.ds(0, TB)], xb.at[:, pl.ds(i * TB, TB)], wsem.at[i])

    pl.run_scoped(phase1,
                  pltpu.VMEM((NV, TB, CN), f32), pltpu.VMEM((TB, CN), f32), pltpu.VMEM((TB, CN), f32),
                  pltpu.VMEM((2, TB, CN), f32), pltpu.VMEM((2, TB, CN), f32), pltpu.VMEM((2, TB, 128), jnp.int32),
                  pltpu.VMEM((TB, 128), f32), pltpu.VMEM((TB, 128), f32), pltpu.VMEM((TB, 128), f32),
                  pltpu.VMEM((TB, 128), f32), pltpu.VMEM((1, TB), f32))

    KD = 2 * ST * NB
    NH = H // TB - REST

    def phase2(xs, od):
        SL = T // (NV // 2)

        def gload(j):
            return lcopy(Gh.at[:, cols(j)], wg.at[:, cols(j)], gsem.at[j])

        def xscopy(h, i):
            return lcopy(X.at[pl.ds(mo(i * SL, SL), SL), pl.ds(mo(h * TB, TB), TB)], xs.at[i % 2], xssem.at[i % 2])

        def odcopy(h, j, s):
            return lcopy(od.at[s], dW.at[pl.ds(mo(h * TB, TB), TB), cols(j)], odsem.at[s])

        gcopy(NB - 1).wait()
        for j in range(NV):
            gload(j).start()
        xscopy(1, 0).start()
        for i in range(T // TB):
            x0copy(i).wait()

        def tr0(i, c):
            gb[:, pl.ds(mo(i * TB, TB), TB)] = xb[:, pl.ds(mo(i * TB, TB), TB)].T
            return c

        lax.fori_loop(0, T // TB, tr0, 0)

        def hstep(h, cur, fut):
            def body(i, c):
                exchange(KD + h * (NV // 2) + i)

                @pl.when(h == 0)
                def _():
                    gload(2 * i).wait()
                    gload(2 * i + 1).wait()

                @pl.when((h > 0) | (i > 0))
                def _():
                    for s in PAIR:
                        odcopy(h, 2 * i + s, s).wait()
                hn = jnp.minimum(h + 1, NH - 1)
                xscopy(hn, i).wait()

                @pl.when((h < NH - 1) | (i < NV // 2 - 1))
                def _():
                    last = i == NV // 2 - 1
                    xscopy(jnp.minimum(jnp.where(last, h + 2, h + 1), NH - 1), jnp.where(last, 0, i + 1)).start()
                for s in PAIR:
                    od[s] = jnp.dot(cur[...], wg[:, cols(2 * i + s)], preferred_element_type=f32).astype(bf16)
                fut[:, pl.ds(mo(i * SL, SL), SL)] = xs[i % 2].T
                for s in PAIR:
                    odcopy(h, 2 * i + s, s).start()
                return c

            lax.fori_loop(0, NV // 2, body, 0)

        def hpair(hh, c):
            hstep(2 * hh, gb, xb)
            hstep(2 * hh + 1, xb, gb)
            return c

        lax.fori_loop(0, NH // 2, hpair, 0)
        for s in PAIR:
            odcopy(NH - 1, NV - 2 + s, s).wait()

    pl.run_scoped(phase2, pltpu.VMEM((2, T // (NV // 2), TB), bf16), pltpu.VMEM((2, TB, CN), bf16))

    KE = KD + NH * (NV // 2)
    KL = K0 + OFFS[-1] + PERIOD * (NU - 1) + 1

    def tail(k, c):
        exchange(k)
        return c

    lax.fori_loop(KE, max(KL, KE), tail, 0)
    u = NU - 1
    for d in PAIR:
        sendA(u, d).wait_send()
        sendB(u, d).wait_send()
        sendC(u, d).wait_send()
        sendG(u, d).wait_send()
        sendR(u, d).wait_send()
        sibG(u, d).wait_send()
    sibO(u).wait_send()
    sibR(u).wait_send()
    ownO(u).wait()

    def sw(u, c):
        sibW(u).wait_recv()
        return c

    lax.fori_loop(0, NU, sw, 0)


def rest(X, Gh, dWa, dXa, dW, dXo, wg, xa, xb, xs, od, cx, cw, gsem, x0sem, xssem, odsem, cxsem, cwsem):
    T, H = X.shape
    V = Gh.shape[1]
    NV = V // CN
    ST = NV // 2
    NH = H // TB
    H0 = NH - REST
    SL = T // ST
    NS = REST * ST
    f32, bf16 = jnp.float32, jnp.bfloat16
    mo = pl.multiple_of
    RX, RW = T // NS, H0 * TB // NS

    def lcopy(src, dst, sem):
        return pltpu.make_async_copy(src, dst, sem)

    def cols(j):
        return pl.ds(mo(j * CN, CN), CN)

    def gload(j):
        return lcopy(Gh.at[:, cols(j)], wg.at[:, cols(j)], gsem.at[j])

    def x0copy(i):
        return lcopy(X.at[pl.ds(i * TB, TB), pl.ds(H0 * TB, TB)], xb.at[:, pl.ds(i * TB, TB)], x0sem.at[i])

    def xscopy(h, i):
        return lcopy(X.at[pl.ds(mo(i * SL, SL), SL), pl.ds(mo(h * TB, TB), TB)], xs.at[i % 2], xssem.at[i % 2])

    def odcopy(h, j, s):
        return lcopy(od.at[s], dW.at[pl.ds(h * TB, TB), cols(j)], odsem.at[s])

    def cin(c):
        return (lcopy(dXa.at[pl.ds(mo(c * RX, RX), RX)], cx.at[c % 2], cxsem.at[0, c % 2]),
                lcopy(dWa.at[pl.ds(mo(c * RW, RW), RW)], cw.at[c % 2], cwsem.at[0, c % 2]))

    def cout(c):
        return (lcopy(cx.at[c % 2], dXo.at[pl.ds(mo(c * RX, RX), RX)], cxsem.at[1, c % 2]),
                lcopy(cw.at[c % 2], dW.at[pl.ds(mo(c * RW, RW), RW)], cwsem.at[1, c % 2]))

    for i in range(T // TB):
        x0copy(i).start()
    for j in PAIR:
        gload(j).start()
    xscopy(H0 + 1, 0).start()
    for x in cin(0):
        x.start()
    for j in range(2, NV):
        gload(j).start()
    for i in range(T // TB):
        x0copy(i).wait()

    def tr0(i, c):
        xa[:, pl.ds(mo(i * TB, TB), TB)] = xb[:, pl.ds(mo(i * TB, TB), TB)].T
        return c

    lax.fori_loop(0, T // TB, tr0, 0)

    def hstep(r, cur, fut):
        h = H0 + r

        def body(i, c):
            q = r * ST + i

            @pl.when(q > 0)
            def _():
                for x in cout(q - 1):
                    x.wait()

            @pl.when(q < NS - 1)
            def _():
                for x in cin(q + 1):
                    x.start()
            for x in cin(q):
                x.wait()
            for x in cout(q):
                x.start()
            if r == 0:
                gload(2 * i).wait()
                gload(2 * i + 1).wait()
            if r < REST - 1:
                xscopy(h + 1, i).wait()

                @pl.when((i < ST - 1) | (r < REST - 2))
                def _():
                    last = i == ST - 1
                    xscopy(jnp.where(last, h + 2, h + 1), jnp.where(last, 0, i + 1)).start()

            @pl.when(q > 0)
            def _():
                for s in PAIR:
                    odcopy(h, 2 * i + s, s).wait()
            for s in PAIR:
                od[s] = jnp.dot(cur[...], wg[:, cols(2 * i + s)], preferred_element_type=f32).astype(bf16)
            if r < REST - 1:
                fut[:, pl.ds(mo(i * SL, SL), SL)] = xs[i % 2].T
            for s in PAIR:
                odcopy(h, 2 * i + s, s).start()
            return c

        lax.fori_loop(0, ST, body, 0)

    for r in range(REST):
        hstep(r, (xa, xb)[r % 2], (xb, xa)[r % 2])
    for s in PAIR:
        odcopy(NH - 1, NV - 2 + s, s).wait()
    for x in cout(NS - 1):
        x.wait()


def solution(mesh):
    n = mesh.shape['tp']

    def local(X, W, labels):
        T, H = X.shape
        V = W.shape[1]
        NB, NV = T // TB, V // CN
        NU, UR = 2 * NB, TB // 2
        HH = H // 2
        QR = UR // (n // 2)
        HR = QR // 2
        lab = jnp.broadcast_to(labels[:, None], (T, 128))
        f32, bf16 = jnp.float32, jnp.bfloat16
        S = jax.ShapeDtypeStruct
        D = pltpu.SemaphoreType.DMA
        hbm = pl.BlockSpec(memory_space=pl.ANY)
        outs = pl.pallas_call(
            functools.partial(kernel, n),
            out_shape=[S((8, 128), f32), S((H - REST * TB, V), bf16), S((T, H), bf16), S((T, V), bf16), S((T, HH), f32),
                       S((2, NU * HR, HH), f32), S((2, NU * HR, HH), f32), S((2, NU * HR, HH), f32)],
            in_specs=[hbm] * 3,
            out_specs=[pl.BlockSpec(memory_space=pltpu.VMEM)] + [hbm] * 7,
            scratch_shapes=[
                pltpu.VMEM((H, V), bf16), pltpu.VMEM((TB, H), bf16), pltpu.VMEM((TB, V), bf16),
                pltpu.VMEM((HH // CN, TB, CN), f32),
                pltpu.VMEM((2, 8, TB), f32), pltpu.VMEM((2, n, 8, TB), f32),
                pltpu.VMEM((2, HR, HH), f32), pltpu.VMEM((2, HR, HH), f32), pltpu.VMEM((2, HR, HH), f32),
                pltpu.VMEM((2, 2, HR, HH), f32), pltpu.VMEM((QR, HH), bf16),
                D((NV,)), D, D, D((NV,)), D((2, n)), D((2, n)), pltpu.SemaphoreType.REGULAR((HH // CN,)),
                D((2,)), D((HH // CN,)), D((2,)), D((2,)), D((2,)),
                D((2,)), D((2, NU)), D((2,)), D((2, NU)), D((2,)), D((2, NU)), D((2,)), D((2, NU)),
                D((2,)), D((2, NU)), D((4,)), D((NU,)), D((10,)), D,
            ],
            compiler_params=pltpu.CompilerParams(collective_id=0, has_side_effects=True,
                                                 vmem_limit_bytes=67043328),
            cost_estimate=pl.CostEstimate(flops=6 * T * H * V, bytes_accessed=8 * T * H, transcendentals=T * V),
        )(X, W, lab)
        ST = NV // 2
        NS = REST * ST
        dW, dX = pl.pallas_call(
            rest,
            out_shape=[S((H, V), bf16), S((T, H), bf16)],
            in_specs=[hbm] * 4,
            out_specs=[hbm] * 2,
            scratch_shapes=[
                pltpu.VMEM((T, V), bf16), pltpu.VMEM((TB, T), bf16), pltpu.VMEM((TB, T), bf16),
                pltpu.VMEM((2, T // ST, TB), bf16), pltpu.VMEM((2, TB, CN), bf16),
                pltpu.VMEM((2, T // NS, H), bf16), pltpu.VMEM((2, (H - REST * TB) // NS, V), bf16),
                D((NV,)), D((T // TB,)), D((2,)), D((2,)), D((2, 2)), D((2, 2)),
            ],
            compiler_params=pltpu.CompilerParams(vmem_limit_bytes=67043328),
            cost_estimate=pl.CostEstimate(flops=2 * T * REST * TB * V, bytes_accessed=10 * T * H, transcendentals=0),
        )(X, outs[3], outs[1], outs[2])
        return outs[0][0, :1], dW, dX

    return jax.shard_map(local, mesh=mesh,
                         in_specs=(P('dp', None), P(None, 'tp'), P('dp')),
                         out_specs=(P('dp'), P('dp', 'tp'), P('dp', None)),
                         check_vma=False)
```
